128 devices in a mesh: dp: 16 (over x_hi, z, core), blk: 8 (over y, x_lo).
Axes of the slice: x: 4 (x_hi: 2, x_lo: 2; x = x_hi * 2 + x_lo), y: 4, z: 4, core: 2. Of those that a mesh axis runs over, the one named last changes fastest.
Arguments:
- inputs: bfloat16 [512, 8192], P('blk', 'dp'), may hold values from -6 to 6
- upstream: bfloat16 [512, 8192], P('blk', 'dp'), may hold values from -1.5 to 1.5
- gate_weight: bfloat16 [8192, 14784], P('dp', 'blk'), may hold values from -0.0625 to 0.0625
- up_weight: bfloat16 [8192, 14784], P('dp', 'blk'), may hold values from -0.0625 to 0.0625
- down_weight: bfloat16 [14784, 8192], P('blk', 'dp'), may hold values from -0.046875 to 0.046875
Outputs:
- input_grad: bfloat16 [512, 8192], P('blk', 'dp')
- gate_grad: bfloat16 [8192, 14784], P('dp', 'blk')
- up_grad: bfloat16 [8192, 14784], P('dp', 'blk')
- down_grad: bfloat16 [14784, 8192], P('blk', 'dp')
The draws below stay inside these ranges and needn't reach their ends.
All inputs are finite; a program needn't handle non-finite values.
Results may differ from the reference program's by a relative error of at most 0.005.
Values may be sent and summed in bfloat16 or wider, within the bound.
A program may use at most 128 MiB of HBM per device.

```python
import jax
import jax.numpy as jnp

D = 8192
FF = 14784
TOKENS = 512


def block_scale(rng, shape, pieces, low, high):
    def one(axis_at, parts):
        steps = jax.random.uniform(jax.random.fold_in(jax.random.fold_in(rng, 6), axis_at), (parts,), jnp.float32, low / len(pieces), high / len(pieces))
        return jnp.repeat(jnp.exp(steps), shape[axis_at] // parts).reshape((-1,) + (1,) * (len(shape) - axis_at - 1))

    factor_of = one(*pieces[0])
    for cut in pieces[1:]:
        factor_of = factor_of * one(*cut)
    return factor_of


def scatter_about(key, extent, width, bound, shards=(), held_as=jnp.bfloat16):
    array = width * jax.random.normal(key, extent, jnp.float32)
    if shards:
        array = array * block_scale(key, extent, shards, -0.22, 0.18)
    return jnp.clip(array, -bound, bound).astype(held_as)


def setup_inputs(seed: int = 0) -> dict:
    splits = jax.random.split(jax.random.key(seed), 6)
    return {
        "inputs": scatter_about(splits[0], (TOKENS, D), 1.0, 6.0, ((0, 8), (1, 16))),
        "upstream": scatter_about(splits[1], (TOKENS, D), 0.25, 1.5, ((0, 8), (1, 16))),
        "gate_weight": scatter_about(splits[2], (D, FF), D ** -0.5, 0.0625, ((0, 16), (1, 8))),
        "up_weight": scatter_about(splits[3], (D, FF), D ** -0.5, 0.0625, ((0, 16), (1, 8))),
        "down_weight": scatter_about(splits[4], (FF, D), FF ** -0.5, 0.046875, ((0, 8), (1, 16))),
    }


def reference(inputs, upstream, gate_weight, up_weight, down_weight):
    gate = jnp.dot(inputs, gate_weight, preferred_element_type=jnp.float32)
    up = jnp.dot(inputs, up_weight, preferred_element_type=jnp.float32)
    back = jnp.dot(upstream, down_weight.T, preferred_element_type=jnp.float32)
    sig = jax.nn.sigmoid(gate)
    hidden = (gate * sig * up).astype(jnp.bfloat16)
    up_delta = (back * gate * sig).astype(jnp.bfloat16)
    gate_delta = (back * up * sig * (1.0 + gate * (1.0 - sig))).astype(jnp.bfloat16)
    down_grad = jnp.dot(hidden.T, upstream, preferred_element_type=jnp.float32).astype(jnp.bfloat16)
    gate_grad = jnp.dot(inputs.T, gate_delta, preferred_element_type=jnp.float32).astype(jnp.bfloat16)
    up_grad = jnp.dot(inputs.T, up_delta, preferred_element_type=jnp.float32).astype(jnp.bfloat16)
    input_grad = jnp.dot(gate_delta, gate_weight.T, preferred_element_type=jnp.float32)
    input_grad = input_grad + jnp.dot(up_delta, up_weight.T, preferred_element_type=jnp.float32)
    return input_grad.astype(jnp.bfloat16), gate_grad, up_grad, down_grad
```

```python
import jax
import jax.numpy as jnp
from jax import lax
from jax.sharding import PartitionSpec as P


def contract_last(left, right):
    return lax.dot_general(
        left, right, (((1,), (1,)), ((), ())), preferred_element_type=jnp.float32
    )


def contract_first(left, right):
    return lax.dot_general(
        left, right, (((0,), (0,)), ((), ())), preferred_element_type=jnp.float32
    )


def elementwise(gate, up, back):
    sig = jax.nn.sigmoid(gate)
    hidden = (gate * sig * up).astype(jnp.bfloat16)
    up_delta = (back * gate * sig).astype(jnp.bfloat16)
    gate_delta = (back * up * sig * (1.0 + gate * (1.0 - sig))).astype(jnp.bfloat16)
    return (hidden, gate_delta, up_delta)


def local(inputs, upstream, gate_weight, up_weight, down_weight):
    both = lax.all_gather(jnp.concatenate([inputs, upstream], 1), "blk", axis=0, tiled=True)
    width = inputs.shape[1]
    rows_all, grads_all = both[:, :width], both[:, width:]
    parts = [
        jnp.dot(rows_all, gate_weight, preferred_element_type=jnp.float32),
        jnp.dot(rows_all, up_weight, preferred_element_type=jnp.float32),
        contract_last(grads_all, down_weight),
    ]
    sums = [lax.psum_scatter(p, "dp", scatter_dimension=0, tiled=True) for p in parts]
    deltas = elementwise(*sums)
    hidden, gate_delta, up_delta = [
        lax.all_gather(d, "dp", axis=0, tiled=True) for d in deltas
    ]
    partial_input = contract_last(gate_delta, gate_weight) + contract_last(up_delta, up_weight)
    parts = partial_input.reshape(8, -1, width)
    input_grad = jnp.sum(lax.all_to_all(parts, "blk", 0, 0, tiled=True), axis=0)
    down_grad = contract_first(hidden, grads_all).astype(jnp.bfloat16)
    gate_grad = contract_first(rows_all, gate_delta).astype(jnp.bfloat16)
    up_grad = contract_first(rows_all, up_delta).astype(jnp.bfloat16)
    return (input_grad.astype(jnp.bfloat16), gate_grad, up_grad, down_grad)


def solution(mesh):
    return jax.shard_map(
        local,
        mesh=mesh,
        in_specs=(P("blk", "dp"), P("blk", "dp"), P("dp", "blk"), P("dp", "blk"), P("blk", "dp")),
        out_specs=(P("blk", "dp"), P("dp", "blk"), P("dp", "blk"), P("blk", "dp")),
        check_vma=False,
    )
```

```python
import jax
import jax.numpy as jnp
from jax import lax
from jax.experimental import pallas as pl
from jax.experimental.pallas import tpu as pltpu
from jax.sharding import PartitionSpec as P

BF = jnp.bfloat16
F32 = jnp.float32
TAIL = 896
HALF = 1024
OFFSETS = (0, 3, 1, 2)


def contract_last(left, right):
    return lax.dot_general(
        left, right, (((1,), (1,)), ((), ())), preferred_element_type=F32
    )


def contract_first(left, right):
    return lax.dot_general(
        left, right, (((0,), (0,)), ((), ())), preferred_element_type=F32
    )


def kernel(
    inputs, upstream, gate_w, up_w, down_w,
    ig_out, deltas_out, rows_out,
    xin, wf, wl, part, rs_in, rs_out, x_in, x_out, tail, deltas, ig_in, ig_send, ig_val,
    loc_sem, w_send, w_recv,
    in_send, in_recv, pair_send, pair_recv,
    rs_ssem, rs_recv, x_send, x_recv,
    g_send, g_recv, gp_send, gp_recv, ig_ssem, ig_rsem,
):
    ff = gate_w.shape[1]
    rest = ff - HALF
    d = inputs.shape[1]
    dp = lax.axis_index("dp")
    blk = lax.axis_index("blk")
    core = lax.rem(dp, 2)
    z = lax.rem(lax.div(dp, 2), 4)
    xh = lax.div(dp, 8)
    y = lax.div(blk, 2)
    xl = lax.rem(blk, 2)

    def at(dp_=None, blk_=None):
        return {"dp": dp if dp_ is None else dp_, "blk": blk if blk_ is None else blk_}

    def dpi(xh_, z_, core_):
        return (xh_ * 4 + z_) * 2 + core_

    def m4(v):
        return lax.rem(v + 4, 4)

    pair = at(dp_=dpi(xh, z, 1 - core))
    zp = at(dp_=dpi(xh, m4(z + 1), core))
    zm = at(dp_=dpi(xh, m4(z - 1), core))
    xo = at(dp_=dpi(1 - xh, z, core))
    xlo = at(blk_=y * 2 + 1 - xl)
    yp = at(blk_=m4(y + 1) * 2 + xl)
    ym = at(blk_=m4(y - 1) * 2 + xl)
    others = [at(blk_=m4(y + o) * 2 + q) for o in (1, 2, 3) for q in (0, 1)]

    def mo(v, n):
        return pl.multiple_of(v, n)

    def send(src, dst, ssem, rsem, dev):
        c = pltpu.make_async_remote_copy(
            src_ref=src, dst_ref=dst, send_sem=ssem, recv_sem=rsem,
            device_id=dev, device_id_type=pl.DeviceIdType.MESH,
        )
        c.start()
        return c

    wf[0, :, TAIL:] = jnp.zeros((2 * d, HALF - TAIL), BF)
    wf[1, :, TAIL:] = jnp.zeros((2 * d, HALF - TAIL), BF)
    wf[2, HALF - 256:, :] = jnp.zeros((256, 2 * d), BF)

    own_in = [
        pltpu.make_async_copy(
            src, xin.at[a, pl.ds(mo(blk * 64, 64), 64), pl.ds(mo(core * d, 512), d)], loc_sem.at[a]
        )
        for a, src in enumerate((inputs, upstream))
    ]
    for c in own_in:
        c.start()

    barrier = pltpu.get_barrier_semaphore()
    peers = [pair, zp, zm, xo, xlo] + others
    for p in peers:
        pl.semaphore_signal(barrier, inc=1, device_id=p, device_id_type=pl.DeviceIdType.MESH)
    pl.semaphore_wait(barrier, len(peers))

    def piece(rows_blk, core_, a=None):
        r = pl.ds(mo(rows_blk * 64, 64), 64)
        c = pl.ds(mo(core_ * d, 512), d)
        return xin.at[:, r, c] if a is None else xin.at[pl.ds(a, 1), r, c]

    sends = []

    def arrived(ref, sem):
        pltpu.make_async_copy(ref, ref, sem).wait()

    for c in own_in:
        c.wait()
    mine = piece(blk, core)
    sends.append(send(mine, mine, in_send.at[0], in_recv.at[0], xlo))
    sends.append(send(mine, mine, in_send.at[1], in_recv.at[1], yp))
    sends.append(send(mine, mine, in_send.at[2], in_recv.at[2], ym))
    sends.append(send(mine, mine, pair_send.at[0], pair_recv.at[0], pair))

    full = [
        pltpu.make_async_copy(src, wl.at[a], loc_sem.at[5 + a])
        for a, src in enumerate((gate_w, up_w))
    ]
    for c in full:
        c.start()
    my_rows = pl.ds(mo(core * d, 512), d)

    def down_copies(keep, give):
        local_ = pltpu.make_async_copy(
            down_w.at[pl.ds(*keep), :], wf.at[2, pl.ds(0, keep[1]), my_rows], loc_sem.at[4]
        )
        away = pltpu.make_async_remote_copy(
            src_ref=down_w.at[pl.ds(*give), :], dst_ref=wf.at[2, pl.ds(0, give[1]), my_rows],
            send_sem=w_send.at[2], recv_sem=w_recv.at[2],
            device_id=pair, device_id_type=pl.DeviceIdType.MESH,
        )
        return local_, away

    def head(a, hbm):
        return hbm.at[:, pl.ds(0, HALF)], wf.at[a, my_rows, :]

    heads = (gate_w, up_w)

    @pl.when(core == 0)
    def _():
        for c in down_copies((0, HALF), (HALF, rest)):
            c.start()
        for a in (0, 1):
            pltpu.make_async_copy(*head(a, heads[a]), loc_sem.at[2 + a]).start()
        for a in (0, 1):
            full[a].wait()
            tail[a, :, TAIL - 128:] = jnp.zeros((d, 128), BF)
            tail[a, :, :rest] = wl[a, :, HALF:]
            send(tail.at[a], wf.at[a, my_rows, pl.ds(0, TAIL)], w_send.at[a], w_recv.at[a], pair)

    @pl.when(core == 1)
    def _():
        for c in down_copies((HALF, rest), (0, HALF)):
            c.start()
        for a in (0, 1):
            src, dst = head(a, heads[a])
            send(src, dst, w_send.at[a], w_recv.at[a], pair)
        for a in (0, 1):
            full[a].wait()
            wf[a, my_rows, TAIL - 128:TAIL] = jnp.zeros((d, 128), BF)
            wf[a, my_rows, :rest] = wl[a, :, HALF:]

    pb = y * 2 + 1 - xl
    other = piece(pb, core)
    arrived(other, in_recv.at[0])
    sends.append(send(other, other, in_send.at[3], in_recv.at[3], yp))
    sends.append(send(other, other, in_send.at[4], in_recv.at[4], ym))
    sends.append(send(other, other, pair_send.at[1], pair_recv.at[1], pair))

    def from_neighbours(q, s_yp, s_ym, base):
        bm = m4(y - 1) * 2 + q
        bp = m4(y + 1) * 2 + q
        arrived(piece(bm, core), in_recv.at[s_yp])
        f = piece(bm, core, 0)
        sends.append(send(f, f, in_send.at[base], in_recv.at[base], yp))
        arrived(piece(bp, core), in_recv.at[s_ym])
        f = piece(bp, core, 1)
        sends.append(send(f, f, in_send.at[base + 1], in_recv.at[base + 1], ym))
        i = base - 5
        sends.append(send(piece(bm, core), piece(bm, core), pair_send.at[2 + i], pair_recv.at[2 + i], pair))
        sends.append(send(piece(bp, core), piece(bp, core), pair_send.at[3 + i], pair_recv.at[3 + i], pair))

    def from_far(q, base, i):
        b2 = m4(y + 2) * 2 + q
        for a in (0, 1):
            arrived(piece(b2, core, a), in_recv.at[base + a])
        sends.append(send(piece(b2, core), piece(b2, core), pair_send.at[i], pair_recv.at[i], pair))

    def wait_pair(k):
        qs = (xl, 1 - xl)
        idx = ((0, 1), (2, 4), (3, 5), (6, 7))[k]
        for q, i in zip(qs, idx):
            ref = piece(m4(y + OFFSETS[k]) * 2 + q, 1 - core)
            arrived(ref, pair_recv.at[i])

    def rows_of(k):
        return mo(m4(y + OFFSETS[k]) * 128, 128)

    def forward(k):
        wait_pair(k)
        r = pl.ds(rows_of(k), 128)
        part[k, 0] = jnp.dot(xin[0, r, :], wf[0], preferred_element_type=F32)
        part[k, 1] = jnp.dot(xin[0, r, :], wf[1], preferred_element_type=F32)
        part[k, 2] = contract_last(xin[1, r, :], wf[2])

    def own(k, zd, half):
        return part[k, :, pl.ds(mo(zd * 32 + half * 16, 16), 16), :]

    def rs_send(k, dr, n, val, dev):
        rs_out[k, dr, n] = val.astype(BF)
        sends.append(send(
            rs_out.at[k, dr, n], rs_in.at[k, dr, n], rs_ssem.at[k, dr, n], rs_recv.at[k, dr, n], dev
        ))

    def reduce_first(k):
        for n, far in ((0, 1), (1, 0)):
            for dr, (sign, dev) in enumerate(((1, zp), (-1, zm))):
                zd = m4(z + 2) if far else m4(z + sign)
                rs_send(k, dr, n, own(k, zd, dr if far else 1 - dr), dev)

    def reduce_next(k):
        for dr, (sign, dev) in enumerate(((1, zp), (-1, zm))):
            arrived(rs_in.at[k, dr, 0], rs_recv.at[k, dr, 0])
            rs_send(k, dr, 2, own(k, m4(z + sign), dr) + rs_in[k, dr, 0].astype(F32), dev)

    def chip_sum(k, q):
        return own(k, z, q) + rs_in[k, q, 2].astype(F32) + rs_in[k, 1 - q, 1].astype(F32)

    def reduce_last(k):
        for n in (1, 2):
            for dr in (0, 1):
                arrived(rs_in.at[k, dr, n], rs_recv.at[k, dr, n])
        x_out[k] = chip_sum(k, 1 - xh).astype(BF)
        sends.append(send(x_out.at[k], x_in.at[k], x_send.at[k], x_recv.at[k], xo))

    def tile(k, z_, xh_, rows=16, core_=None):
        c = core if core_ is None else core_
        return deltas.at[
            :,
            pl.ds(mo(rows_of(k) + z_ * 32 + xh_ * 16, 16), rows),
            pl.ds(mo(c * HALF, HALF), HALF),
        ]

    def g_out(k, n, t, rsem, dev):
        sends.append(send(t, t, g_send.at[k, n], g_recv.at[k, rsem], dev))

    def g_pair(k, n, z_):
        t = tile(k, z_, 0, 32)
        sends.append(send(t, t, gp_send.at[k, n], gp_recv.at[k, n], pair))

    def elementwise(k):
        arrived(x_in.at[k], x_recv.at[k])
        sums = chip_sum(k, xh) + x_in[k].astype(F32)
        gate, up, back = sums[0], sums[1], sums[2]
        sig = 1.0 / (1.0 + jnp.exp(-gate))
        gs = gate * sig
        hidden = gs * up
        up_delta = back * gs
        gate_delta = back * up * sig * (1.0 + gate * (1.0 - sig))
        r = pl.ds(mo(rows_of(k) + z * 32 + xh * 16, 16), 16)
        c = pl.ds(mo(core * HALF, HALF), HALF)
        deltas[0, r, c] = hidden.astype(BF)
        deltas[1, r, c] = gate_delta.astype(BF)
        deltas[2, r, c] = up_delta.astype(BF)
        t = tile(k, z, xh)
        g_out(k, 0, t, 0, xo)
        g_out(k, 1, t, 1 + xh, zp)
        g_out(k, 2, t, 3 + xh, zm)

    def gather_x(k):
        t = tile(k, z, 1 - xh)
        arrived(t, g_recv.at[k, 0])
        g_out(k, 3, t, 1 + 1 - xh, zp)
        g_out(k, 4, t, 3 + 1 - xh, zm)
        g_pair(k, 0, z)

    def neighbour_tile(k, xq, n):
        for i, zz in enumerate((m4(z - 1), m4(z + 1))):
            arrived(tile(k, zz, xq), g_recv.at[k, 1 + 2 * i + xq])
        src = tile(k, m4(z - 1 + 2 * xq), xq)
        dev = at(dp_=dpi(xh, m4(z + 1 - 2 * xq), core))
        g_out(k, n, src, 5 + xq, dev)

    def gather_near(k):
        neighbour_tile(k, xh, 5)

    def gather_next(k):
        neighbour_tile(k, 1 - xh, 6)
        g_pair(k, 1, m4(z - 1))
        g_pair(k, 2, m4(z + 1))

    def gather_far(k):
        for q in (0, 1):
            arrived(tile(k, m4(z + 2), q), g_recv.at[k, 5 + q])
        g_pair(k, 3, m4(z + 2))

    outs = []

    def backward(k):
        for n, zz in enumerate((z, m4(z - 1), m4(z + 1), m4(z + 2))):
            arrived(tile(k, zz, 0, 32, 1 - core), gp_recv.at[k, n])
        r = pl.ds(rows_of(k), 128)
        c = pltpu.make_async_copy(deltas.at[:, r, :], deltas_out.at[:, r, :], loc_sem.at[7 + k])
        c.start()
        outs.append(c)
        ig = contract_last(deltas[1, r, :ff], wl[0]) + contract_last(deltas[2, r, :ff], wl[1])
        if k == 0:
            ig_val[...] = ig
            ig_send[k] = ig.astype(BF)
            q = 1 - xl
            sends.append(send(
                ig_send.at[k, pl.ds(mo(q * 64, 64), 64)], ig_in.at[xl],
                ig_ssem.at[k, 0], ig_rsem.at[xl], at(blk_=y * 2 + q),
            ))
        else:
            ig_send[k] = ig.astype(BF)
            for q in (0, 1):
                sends.append(send(
                    ig_send.at[k, pl.ds(q * 64, 64)], ig_in.at[2 * k + xl],
                    ig_ssem.at[k, q], ig_rsem.at[2 * k + xl], at(blk_=m4(y + OFFSETS[k]) * 2 + q),
                ))

    def ready_weights():
        their_rows = pl.ds(mo((1 - core) * d, 512), d)

        def settle(keep, give):
            local_, away = down_copies(keep, give)
            local_.wait()
            away.wait_send()
            arrived(wf.at[2, pl.ds(0, keep[1]), their_rows], w_recv.at[2])

        @pl.when(core == 0)
        def _():
            settle((0, HALF), (HALF, rest))
            for a in (0, 1):
                pltpu.make_async_copy(*head(a, heads[a]), loc_sem.at[2 + a]).wait()
                arrived(wf.at[a, their_rows, :], w_recv.at[a])
                arrived(tail.at[a], w_send.at[a])

        @pl.when(core == 1)
        def _():
            settle((HALF, rest), (0, HALF))
            for a in (0, 1):
                arrived(wf.at[a, their_rows, pl.ds(0, TAIL)], w_recv.at[a])
                arrived(wf.at[a, my_rows, :], w_send.at[a])

    from_neighbours(xl, 1, 2, 5)
    ready_weights()
    forward(0)
    reduce_first(0)
    from_neighbours(1 - xl, 3, 4, 7)
    forward(1)
    reduce_first(1)
    reduce_next(0)
    forward(2)
    reduce_first(2)
    from_far(xl, 5, 6)
    from_far(1 - xl, 7, 7)
    reduce_next(1)
    forward(3)
    reduce_first(3)
    reduce_last(0)
    c = pltpu.make_async_copy(xin.at[:, :, pl.ds(mo(core * d, 512), d)], rows_out, loc_sem.at[11])
    c.start()
    outs.append(c)
    chain = [
        reduce_next, reduce_last, elementwise, gather_x, gather_near, gather_next, gather_far, backward,
    ]
    done = [2, 1, 0, 0]
    for tick in range(len(chain) + 3):
        for k in range(4):
            i = tick - k
            if 0 <= i < len(chain) and i >= done[k]:
                chain[i](k)

    for k in range(4):
        for q in (0, 1):
            i = 2 * k + (q if k else 0)
            if k == 0:
                if q == 0:
                    arrived(ig_in.at[1 - xl], ig_rsem.at[1 - xl])
            else:
                arrived(ig_in.at[i], ig_rsem.at[i])
    total = ig_val[pl.ds(mo(xl * 64, 64), 64), :] + ig_in[1 - xl].astype(F32)
    for i in range(2, 8):
        total = total + ig_in[i].astype(F32)
    ig_out[...] = total.astype(BF)
    for c in sends:
        c.wait_send()
    for c in outs:
        c.wait()


def fused(inputs, upstream, gate_w, up_w, down_w):
    d = inputs.shape[1]
    any_ = pl.BlockSpec(memory_space=pl.ANY)
    dma = pltpu.SemaphoreType.DMA
    return pl.pallas_call(
        kernel,
        name="fused",
        out_shape=(
            jax.ShapeDtypeStruct((64, d), BF),
            jax.ShapeDtypeStruct((3, 512, 2 * HALF), BF),
            jax.ShapeDtypeStruct((2, 512, d), BF),
        ),
        in_specs=[any_] * 5,
        out_specs=(pl.BlockSpec(memory_space=pltpu.VMEM), any_, any_),
        scratch_shapes=[
            pltpu.VMEM((2, 512, 2 * d), BF),
            pltpu.VMEM((3, HALF, HALF), BF),
            pltpu.VMEM((2, d, gate_w.shape[1]), BF),
            pltpu.VMEM((4, 3, 128, HALF), F32),
            pltpu.VMEM((4, 2, 3, 3, 16, HALF), BF),
            pltpu.VMEM((4, 2, 3, 3, 16, HALF), BF),
            pltpu.VMEM((4, 3, 16, HALF), BF),
            pltpu.VMEM((4, 3, 16, HALF), BF),
            pltpu.VMEM((2, d, TAIL), BF),
            pltpu.VMEM((3, 512, 2 * HALF), BF),
            pltpu.VMEM((8, 64, d), BF),
            pltpu.VMEM((4, 128, d), BF),
            pltpu.VMEM((128, d), F32),
            dma((12,)), dma((3,)), dma((3,)),
            dma((9,)), dma((9,)), dma((8,)), dma((8,)),
            dma((4, 2, 3)), dma((4, 2, 3)), dma((4,)), dma((4,)),
            dma((4, 7)), dma((4, 7)), dma((4, 4)), dma((4, 4)), dma((4, 2)), dma((8,)),
        ],
        compiler_params=pltpu.CompilerParams(
            collective_id=0, has_side_effects=True, vmem_limit_bytes=60 * 1024 * 1024
        ),
        cost_estimate=pl.CostEstimate(flops=5 * 10**9, bytes_accessed=20 * 10**6, transcendentals=10**6),
    )(inputs, upstream, gate_w, up_w, down_w)


def grads_kernel(rows, deltas, gate_ref, up_ref, down_ref):
    gate_ref[...] = contract_first(rows[0], deltas[1]).astype(BF)
    up_ref[...] = contract_first(rows[0], deltas[2]).astype(BF)
    down_ref[...] = contract_first(deltas[0], rows[1]).astype(BF)


def weight_grads(rows, deltas, ff):
    d = rows.shape[2]
    n = 512
    return pl.pallas_call(
        grads_kernel,
        name="weight_grads",
        grid=(pl.cdiv(ff, n),),
        out_shape=(
            jax.ShapeDtypeStruct((d, ff), BF),
            jax.ShapeDtypeStruct((d, ff), BF),
            jax.ShapeDtypeStruct((ff, d), BF),
        ),
        in_specs=[
            pl.BlockSpec((2, 512, d), lambda i: (0, 0, 0)),
            pl.BlockSpec((3, 512, n), lambda i: (0, 0, i)),
        ],
        out_specs=(
            pl.BlockSpec((d, n), lambda i: (0, i)),
            pl.BlockSpec((d, n), lambda i: (0, i)),
            pl.BlockSpec((n, d), lambda i: (i, 0)),
        ),
        compiler_params=pltpu.CompilerParams(vmem_limit_bytes=40 * 1024 * 1024),
    )(rows, deltas)


def local(inputs, upstream, gate_weight, up_weight, down_weight):
    input_grad, deltas, rows = fused(inputs, upstream, gate_weight, up_weight, down_weight)
    gate_grad, up_grad, down_grad = weight_grads(rows, deltas, gate_weight.shape[1])
    return (input_grad, gate_grad, up_grad, down_grad)


def solution(mesh):
    return jax.shard_map(
        local,
        mesh=mesh,
        in_specs=(P("blk", "dp"), P("blk", "dp"), P("dp", "blk"), P("dp", "blk"), P("blk", "dp")),
        out_specs=(P("blk", "dp"), P("dp", "blk"), P("dp", "blk"), P("blk", "dp")),
        check_vma=False,
    )
```

```python
import functools

import jax
import jax.numpy as jnp
from jax import lax
from jax.experimental import pallas as pl
from jax.experimental.pallas import tpu as pltpu
from jax.sharding import PartitionSpec as P

BF = jnp.bfloat16
F32 = jnp.float32
HALF = 1024
REST = 896
OFFSETS = (0, 3, 1, 2)


def contract_last(left, right):
    return lax.dot_general(
        left, right, (((1,), (1,)), ((), ())), preferred_element_type=F32
    )


def contract_first(left, right):
    return lax.dot_general(
        left, right, (((0,), (0,)), ((), ())), preferred_element_type=F32
    )


def dot(left, right):
    return jnp.dot(left, right, preferred_element_type=F32)


def kernel(
    inputs, upstream, gate_w, up_w, down_w,
    ig_out, deltas_out, rows_out,
    xin, wf, wl, part, rs_in, rs_out, x_in, x_out, deltas, ig_in, ig_send, ig_val,
    loc_sem, w_send, w_recv,
    in_send, in_recv, pair_send, pair_recv,
    rs_ssem, rs_recv, x_send, x_recv,
    g_send, g_recv, gp_send, gp_recv, ig_ssem, ig_rsem,
):
    ff = gate_w.shape[0]
    rest = ff - HALF
    d = inputs.shape[1]
    dp = lax.axis_index("dp")
    blk = lax.axis_index("blk")
    core = lax.rem(dp, 2)
    z = lax.rem(lax.div(dp, 2), 4)
    xh = lax.div(dp, 8)
    y = lax.div(blk, 2)
    xl = lax.rem(blk, 2)

    def at(dp_=None, blk_=None):
        return {"dp": dp if dp_ is None else dp_, "blk": blk if blk_ is None else blk_}

    def dpi(xh_, z_, core_):
        return (xh_ * 4 + z_) * 2 + core_

    def m4(v):
        return lax.rem(v + 4, 4)

    pair = at(dp_=dpi(xh, z, 1 - core))
    zp = at(dp_=dpi(xh, m4(z + 1), core))
    zm = at(dp_=dpi(xh, m4(z - 1), core))
    xo = at(dp_=dpi(1 - xh, z, core))
    xlo = at(blk_=y * 2 + 1 - xl)
    yp = at(blk_=m4(y + 1) * 2 + xl)
    ym = at(blk_=m4(y - 1) * 2 + xl)
    others = [at(blk_=m4(y + o) * 2 + q) for o in (1, 2, 3) for q in (0, 1)]

    def mo(v, n):
        return pl.multiple_of(v, n)

    def send(src, dst, ssem, rsem, dev):
        c = pltpu.make_async_remote_copy(
            src_ref=src, dst_ref=dst, send_sem=ssem, recv_sem=rsem,
            device_id=dev, device_id_type=pl.DeviceIdType.MESH,
        )
        c.start()
        return c

    for a in range(3):
        wf[a, HALF - 256:, :] = jnp.zeros((256, 2 * d), BF)

    own_in = [
        pltpu.make_async_copy(
            src, xin.at[a, pl.ds(mo(blk * 64, 64), 64), pl.ds(mo(core * d, 512), d)], loc_sem.at[a]
        )
        for a, src in enumerate((inputs, upstream))
    ]
    for c in own_in:
        c.start()

    barrier = pltpu.get_barrier_semaphore()
    peers = [pair, zp, zm, xo, xlo] + others
    for p in peers:
        pl.semaphore_signal(barrier, inc=1, device_id=p, device_id_type=pl.DeviceIdType.MESH)
    pl.semaphore_wait(barrier, len(peers))

    def piece(rows_blk, core_, a=None):
        r = pl.ds(mo(rows_blk * 64, 64), 64)
        c = pl.ds(mo(core_ * d, 512), d)
        return xin.at[:, r, c] if a is None else xin.at[pl.ds(a, 1), r, c]

    sends = []
    part_sends = []

    def arrived(ref, sem):
        pltpu.make_async_copy(ref, ref, sem).wait()

    for c in own_in:
        c.wait()
    mine = piece(blk, core)
    sends.append(send(mine, mine, in_send.at[0], in_recv.at[0], xlo))
    sends.append(send(mine, mine, in_send.at[1], in_recv.at[1], yp))
    sends.append(send(mine, mine, in_send.at[2], in_recv.at[2], ym))
    sends.append(send(mine, mine, pair_send.at[0], pair_recv.at[0], pair))

    hbm = (gate_w, up_w, down_w)
    full = [
        pltpu.make_async_copy(hbm[a], wl.at[a], loc_sem.at[5 + a]) for a in (0, 1)
    ]
    my_rows = pl.ds(mo(core * d, 512), d)
    their_rows = pl.ds(mo((1 - core) * d, 512), d)

    def weight_copies(a, keep, give):
        local_ = pltpu.make_async_copy(
            hbm[a].at[pl.ds(*keep), :], wf.at[a, pl.ds(0, keep[1]), my_rows], loc_sem.at[2 + a]
        )
        away = pltpu.make_async_remote_copy(
            src_ref=hbm[a].at[pl.ds(*give), :], dst_ref=wf.at[a, pl.ds(0, give[1]), my_rows],
            send_sem=w_send.at[a], recv_sem=w_recv.at[a],
            device_id=pair, device_id_type=pl.DeviceIdType.MESH,
        )
        return local_, away

    def on_core(body):
        for c_, args in enumerate((((0, HALF), (HALF, rest)), ((HALF, rest), (0, HALF)))):
            pl.when(core == c_)(functools.partial(body, *args))

    def start_weights(keep, give):
        for a in range(3):
            for c in weight_copies(a, keep, give):
                c.start()

    on_core(start_weights)
    for c in full:
        c.start()

    pb = y * 2 + 1 - xl
    other = piece(pb, core)
    arrived(other, in_recv.at[0])
    sends.append(send(other, other, in_send.at[3], in_recv.at[3], yp))
    sends.append(send(other, other, in_send.at[4], in_recv.at[4], ym))
    sends.append(send(other, other, pair_send.at[1], pair_recv.at[1], pair))

    def from_neighbours(q, s_yp, s_ym, base):
        bm = m4(y - 1) * 2 + q
        bp = m4(y + 1) * 2 + q
        arrived(piece(bm, core), in_recv.at[s_yp])
        f = piece(bm, core, 0)
        sends.append(send(f, f, in_send.at[base], in_recv.at[base], yp))
        arrived(piece(bp, core), in_recv.at[s_ym])
        f = piece(bp, core, 1)
        sends.append(send(f, f, in_send.at[base + 1], in_recv.at[base + 1], ym))
        i = base - 5
        sends.append(send(piece(bm, core), piece(bm, core), pair_send.at[2 + i], pair_recv.at[2 + i], pair))
        sends.append(send(piece(bp, core), piece(bp, core), pair_send.at[3 + i], pair_recv.at[3 + i], pair))

    def from_far(q, base, i):
        b2 = m4(y + 2) * 2 + q
        for a in (0, 1):
            arrived(piece(b2, core, a), in_recv.at[base + a])
        sends.append(send(piece(b2, core), piece(b2, core), pair_send.at[i], pair_recv.at[i], pair))

    def wait_pair(k):
        qs = (xl, 1 - xl)
        idx = ((0, 1), (2, 4), (3, 5), (6, 7))[k]
        for q, i in zip(qs, idx):
            ref = piece(m4(y + OFFSETS[k]) * 2 + q, 1 - core)
            arrived(ref, pair_recv.at[i])

    def rows_of(k):
        return mo(m4(y + OFFSETS[k]) * 128, 128)

    def forward(k):
        wait_pair(k)
        r = pl.ds(rows_of(k), 128)
        part[k, 0] = contract_last(xin[0, r, :], wf[0])
        part[k, 1] = contract_last(xin[0, r, :], wf[1])
        part[k, 2] = contract_last(xin[1, r, :], wf[2])

    def own(k, zd, half):
        return part[k, :, pl.ds(mo(zd * 32 + half * 16, 16), 16), :]

    def each_width(body):
        for c_, width in enumerate((HALF, REST)):
            pl.when(core == c_)(functools.partial(body, c_, width))

    def send_part(src, dst, ssem, rsem, dev):
        def copy(c_, width):
            return pltpu.make_async_remote_copy(
                src_ref=src(c_, width), dst_ref=dst(c_, width), send_sem=ssem, recv_sem=rsem,
                device_id=dev, device_id_type=pl.DeviceIdType.MESH,
            )

        each_width(lambda c_, width: copy(c_, width).start())
        part_sends.append(copy)

    def part_arrived(ref, sem):
        each_width(lambda c_, width: arrived(ref(c_, width), sem))

    def lanes(ref):
        return lambda c_, width: ref.at[:, :, pl.ds(0, width)]

    def rs_send(k, dr, n, val, dev):
        rs_out[k, dr, n] = val.astype(BF)
        send_part(
            lanes(rs_out.at[k, dr, n]), lanes(rs_in.at[k, dr, n]),
            rs_ssem.at[k, dr, n], rs_recv.at[k, dr, n], dev,
        )

    def reduce_first(k):
        for n, far in ((0, 1), (1, 0)):
            for dr, (sign, dev) in enumerate(((1, zp), (-1, zm))):
                zd = m4(z + 2) if far else m4(z + sign)
                rs_send(k, dr, n, own(k, zd, dr if far else 1 - dr), dev)

    def reduce_next(k):
        for dr, (sign, dev) in enumerate(((1, zp), (-1, zm))):
            part_arrived(lanes(rs_in.at[k, dr, 0]), rs_recv.at[k, dr, 0])
            rs_send(k, dr, 2, own(k, m4(z + sign), dr) + rs_in[k, dr, 0].astype(F32), dev)

    def chip_sum(k, q):
        return own(k, z, q) + rs_in[k, q, 2].astype(F32) + rs_in[k, 1 - q, 1].astype(F32)

    def reduce_last(k):
        for n in (1, 2):
            for dr in (0, 1):
                part_arrived(lanes(rs_in.at[k, dr, n]), rs_recv.at[k, dr, n])
        x_out[k] = chip_sum(k, 1 - xh).astype(BF)
        send_part(lanes(x_out.at[k]), lanes(x_in.at[k]), x_send.at[k], x_recv.at[k], xo)

    def tile(k, z_, xh_, rows=16):
        r = pl.ds(mo(rows_of(k) + z_ * 32 + xh_ * 16, 16), rows)
        return lambda c_, width: deltas.at[:, r, pl.ds(c_ * HALF, width)]

    def g_out(k, n, t, rsem, dev):
        send_part(t, t, g_send.at[k, n], g_recv.at[k, rsem], dev)

    def g_pair(k, n, z_):
        t = tile(k, z_, 0, 32)
        send_part(t, t, gp_send.at[k, n], gp_recv.at[k, n], pair)

    def elementwise(k):
        part_arrived(lanes(x_in.at[k]), x_recv.at[k])
        sums = chip_sum(k, xh) + x_in[k].astype(F32)
        gate, up, back = sums[0], sums[1], sums[2]
        sig = 1.0 / (1.0 + jnp.exp(-gate))
        gs = gate * sig
        hidden = gs * up
        up_delta = back * gs
        gate_delta = back * up * sig * (1.0 + gate * (1.0 - sig))
        r = pl.ds(mo(rows_of(k) + z * 32 + xh * 16, 16), 16)
        c = pl.ds(mo(core * HALF, HALF), HALF)
        deltas[0, r, c] = hidden.astype(BF)
        deltas[1, r, c] = gate_delta.astype(BF)
        deltas[2, r, c] = up_delta.astype(BF)
        t = tile(k, z, xh)
        g_out(k, 0, t, 0, xo)
        g_out(k, 1, t, 1 + xh, zp)
        g_out(k, 2, t, 3 + xh, zm)

    def gather_x(k):
        t = tile(k, z, 1 - xh)
        part_arrived(t, g_recv.at[k, 0])
        g_out(k, 3, t, 1 + 1 - xh, zp)
        g_out(k, 4, t, 3 + 1 - xh, zm)
        g_pair(k, 0, z)

    def neighbour_tile(k, xq, n):
        for i, zz in enumerate((m4(z - 1), m4(z + 1))):
            part_arrived(tile(k, zz, xq), g_recv.at[k, 1 + 2 * i + xq])
        src = tile(k, m4(z - 1 + 2 * xq), xq)
        dev = at(dp_=dpi(xh, m4(z + 1 - 2 * xq), core))
        g_out(k, n, src, 5 + xq, dev)

    def gather_near(k):
        neighbour_tile(k, xh, 5)

    def gather_next(k):
        neighbour_tile(k, 1 - xh, 6)
        g_pair(k, 1, m4(z - 1))
        g_pair(k, 2, m4(z + 1))

    def gather_far(k):
        for q in (0, 1):
            part_arrived(tile(k, m4(z + 2), q), g_recv.at[k, 5 + q])
        g_pair(k, 3, m4(z + 2))

    outs = []

    def backward(k):
        for n, zz in enumerate((z, m4(z - 1), m4(z + 1), m4(z + 2))):
            t = tile(k, zz, 0, 32)
            pl.when(core == 0)(lambda: arrived(t(1, REST), gp_recv.at[k, n]))
            pl.when(core == 1)(lambda: arrived(t(0, HALF), gp_recv.at[k, n]))
        r = pl.ds(rows_of(k), 128)
        c = pltpu.make_async_copy(deltas.at[:, r, :], deltas_out.at[:, r, :], loc_sem.at[7 + k])
        c.start()
        outs.append(c)
        ig = dot(deltas[1, r, :ff], wl[0]) + dot(deltas[2, r, :ff], wl[1])
        if k == 0:
            ig_val[...] = ig
            ig_send[k] = ig.astype(BF)
            q = 1 - xl
            sends.append(send(
                ig_send.at[k, pl.ds(mo(q * 64, 64), 64)], ig_in.at[xl],
                ig_ssem.at[k, 0], ig_rsem.at[xl], at(blk_=y * 2 + q),
            ))
        else:
            ig_send[k] = ig.astype(BF)
            for q in (0, 1):
                sends.append(send(
                    ig_send.at[k, pl.ds(q * 64, 64)], ig_in.at[2 * k + xl],
                    ig_ssem.at[k, q], ig_rsem.at[2 * k + xl], at(blk_=m4(y + OFFSETS[k]) * 2 + q),
                ))

    def ready_weights():
        def settle(keep, give):
            for a in range(3):
                local_, away = weight_copies(a, keep, give)
                local_.wait()
                away.wait_send()
                arrived(wf.at[a, pl.ds(0, keep[1]), their_rows], w_recv.at[a])

        on_core(settle)

    from_neighbours(xl, 1, 2, 5)
    ready_weights()
    forward(0)
    reduce_first(0)
    from_neighbours(1 - xl, 3, 4, 7)
    forward(1)
    reduce_first(1)
    reduce_next(0)
    forward(2)
    reduce_first(2)
    from_far(xl, 5, 6)
    from_far(1 - xl, 7, 7)
    reduce_next(1)
    forward(3)
    reduce_first(3)
    reduce_last(0)
    for c in full:
        c.wait()
    c = pltpu.make_async_copy(xin.at[:, :, pl.ds(mo(core * d, 512), d)], rows_out, loc_sem.at[11])
    c.start()
    outs.append(c)
    chain = [
        reduce_next, reduce_last, elementwise, gather_x, gather_near, gather_next, gather_far, backward,
    ]
    done = [2, 1, 0, 0]
    for tick in range(len(chain) + 3):
        for k in range(4):
            i = tick - k
            if 0 <= i < len(chain) and i >= done[k]:
                chain[i](k)

    for k in range(4):
        for q in (0, 1):
            i = 2 * k + (q if k else 0)
            if k == 0:
                if q == 0:
                    arrived(ig_in.at[1 - xl], ig_rsem.at[1 - xl])
            else:
                arrived(ig_in.at[i], ig_rsem.at[i])
    total = ig_val[pl.ds(mo(xl * 64, 64), 64), :] + ig_in[1 - xl].astype(F32)
    for i in range(2, 8):
        total = total + ig_in[i].astype(F32)
    ig_out[...] = total.astype(BF)
    for c in sends:
        c.wait_send()
    for copy in part_sends:
        each_width(lambda c_, width: copy(c_, width).wait_send())
    for c in outs:
        c.wait()


def fused(inputs, upstream, gate_w, up_w, down_w):
    d = inputs.shape[1]
    any_ = pl.BlockSpec(memory_space=pl.ANY)
    dma = pltpu.SemaphoreType.DMA
    return pl.pallas_call(
        kernel,
        name="fused",
        out_shape=(
            jax.ShapeDtypeStruct((64, d), BF),
            jax.ShapeDtypeStruct((3, 512, 2 * HALF), BF),
            jax.ShapeDtypeStruct((2, 512, d), BF),
        ),
        in_specs=[any_] * 5,
        out_specs=(pl.BlockSpec(memory_space=pltpu.VMEM), any_, any_),
        scratch_shapes=[
            pltpu.VMEM((2, 512, 2 * d), BF),
            pltpu.VMEM((3, HALF, HALF), BF),
            pltpu.VMEM((2, gate_w.shape[0], d), BF),
            pltpu.VMEM((4, 3, 128, HALF), F32),
            pltpu.VMEM((4, 2, 3, 3, 16, HALF), BF),
            pltpu.VMEM((4, 2, 3, 3, 16, HALF), BF),
            pltpu.VMEM((4, 3, 16, HALF), BF),
            pltpu.VMEM((4, 3, 16, HALF), BF),
            pltpu.VMEM((3, 512, 2 * HALF), BF),
            pltpu.VMEM((8, 64, d), BF),
            pltpu.VMEM((4, 128, d), BF),
            pltpu.VMEM((128, d), F32),
            dma((12,)), dma((3,)), dma((3,)),
            dma((9,)), dma((9,)), dma((8,)), dma((8,)),
            dma((4, 2, 3)), dma((4, 2, 3)), dma((4,)), dma((4,)),
            dma((4, 7)), dma((4, 7)), dma((4, 4)), dma((4, 4)), dma((4, 2)), dma((8,)),
        ],
        compiler_params=pltpu.CompilerParams(
            collective_id=0, has_side_effects=True, vmem_limit_bytes=60 * 1024 * 1024
        ),
        cost_estimate=pl.CostEstimate(flops=5 * 10**9, bytes_accessed=20 * 10**6, transcendentals=10**6),
    )(inputs, upstream, gate_w, up_w, down_w)


def grads_kernel(rows, deltas, gate_ref, up_ref, down_ref):
    gate_ref[...] = contract_first(deltas[1], rows[0]).astype(BF)
    up_ref[...] = contract_first(deltas[2], rows[0]).astype(BF)
    down_ref[...] = contract_first(deltas[0], rows[1]).astype(BF)


def weight_grads(rows, deltas, ff):
    d = rows.shape[2]
    n = 512
    return pl.pallas_call(
        grads_kernel,
        name="weight_grads",
        grid=(pl.cdiv(ff, n),),
        out_shape=(jax.ShapeDtypeStruct((ff, d), BF),) * 3,
        in_specs=[
            pl.BlockSpec((2, 512, d), lambda i: (0, 0, 0)),
            pl.BlockSpec((3, 512, n), lambda i: (0, 0, i)),
        ],
        out_specs=(pl.BlockSpec((n, d), lambda i: (i, 0)),) * 3,
        compiler_params=pltpu.CompilerParams(vmem_limit_bytes=62 * 1024 * 1024),
    )(rows, deltas)


def local(inputs, upstream, gate_weight, up_weight, down_weight):
    input_grad, deltas, rows = fused(inputs, upstream, gate_weight.T, up_weight.T, down_weight)
    gate_grad, up_grad, down_grad = weight_grads(rows, deltas, down_weight.shape[0])
    return (input_grad, gate_grad.T, up_grad.T, down_grad)


def solution(mesh):
    return jax.shard_map(
        local,
        mesh=mesh,
        in_specs=(P("blk", "dp"), P("blk", "dp"), P("dp", "blk"), P("dp", "blk"), P("blk", "dp")),
        out_specs=(P("blk", "dp"), P("dp", "blk"), P("dp", "blk"), P("blk", "dp")),
        check_vma=False,
    )
```
